32 devices in a mesh: rep: 2 (over y), dp: 16 (over z, x, core).
Axes of the slice: x: 2, y: 2, z: 4, core: 2. Of those that a mesh axis runs over, the one named last changes fastest.
Arguments:
- hidden: bfloat16 [256, 2, 3584], P(('rep', 'dp')), may hold values from -96 to 96
- lm_head: bfloat16 [3584, 12288], P(None, ('rep', 'dp')), may hold values from -0.3125 to 0.3125
- reward_head: bfloat16 [3584], replicated, may hold values from -0.09375 to 0.09375
- target_ids: int32 [256, 2], P(('rep', 'dp')), may hold values from 0 to 12287
- lengths: int32 [256], P(('rep', 'dp')), may hold values from 1 to 2
- prompt_ids: int32 [256], P(('rep', 'dp')), may hold values from 0 to 15, as said below
Outputs:
- token_logprobs: float32 [256, 2], P(('rep', 'dp'))
- advantages: float32 [256], P(('rep', 'dp'))
The draws below stay inside these ranges and needn't reach their ends.
Inputs may be any that keep to these rules, and one draw needn't show every extreme that they name: `prompt_ids`: each prompt id names exactly 16 responses.
All inputs are finite; a program needn't handle non-finite values.
Results may differ from the reference program's by a relative error of at most 0.0003.
Values may be sent and summed in bfloat16 or wider, within the bound.
No kernel may reach another device: no remote copies, remote signals or barrier semaphores. Data moves between devices by JAX's collectives and lax.ppermute only.
A program may use at most 128 MiB of HBM per device.

```python
import jax
import jax.numpy as jnp
from jax import lax

D = 3584
VOC_DEV = 384
GROUP = 16
WIN = 2
VOCAB = 12288
PROMPTS = 16
RESPONSES = 256
TOKENS = 512


def draw_hidden(key, part):
    base = jax.random.truncated_normal(key, -6.0, 6.0, (RESPONSES, WIN, D), jnp.float32)
    return base.astype(jnp.bfloat16)


def draw_prompt_ids(key, part):
    order = jax.random.permutation(jax.random.fold_in(key, 5), RESPONSES)
    return (order // GROUP).astype(jnp.int32)


def plant(entries, key, smallest, top_value):
    longest = entries.shape.index(max(entries.shape))
    spots = []
    for shift in (0, 1):
        where = [jax.random.randint(jax.random.fold_in(key, axis), (), 0, length) for axis, length in enumerate(entries.shape)]
        where[longest] = (where[longest] + shift) % entries.shape[longest]
        spots.append(tuple(where))
    return entries.at[spots[0]].set(smallest).at[spots[1]].set(top_value)


def levels(own_key, extent, split, low, top_value):
    level = 1.0
    for position, blocks in split:
        heights = jax.random.uniform(jax.random.fold_in(jax.random.fold_in(own_key, 6), position), (blocks,), jnp.float32, low / len(split), top_value / len(split))
        level = level * jnp.repeat(jnp.exp(heights), extent[position] // blocks).reshape((-1,) + (1,) * (len(extent) - 1 - position))
    return level


def centred(rng, extent, scale, limit, pieces=(), kind=jnp.bfloat16):
    array = jax.random.normal(rng, extent, jnp.float32) * scale
    if len(pieces) > 0:
        array = levels(rng, extent, pieces, -0.22, 0.18) * array
    return jnp.clip(array, min=-limit, max=limit).astype(kind)


def setup_inputs(seed: int = 0) -> dict:
    keys = jax.random.split(jax.random.key(seed), 7)
    hidden = draw_hidden(jax.random.fold_in(keys[6], 71), 0)
    lm_head = centred(keys[1], (D, VOCAB), (D // 9) ** -0.5, 0.3125, ((1, 32),))
    reward_head = centred(keys[2], (D,), D ** -0.5, 0.09375)
    target_ids = plant(jax.random.randint(keys[3], (RESPONSES, WIN), 0, VOCAB), jax.random.fold_in(keys[3], 1), 0, VOCAB - 1).astype(jnp.int32)
    lengths = plant(jax.random.randint(keys[4], (RESPONSES,), 1, WIN + 1), jax.random.fold_in(keys[4], 1), 1, WIN).astype(jnp.int32)
    prompt_ids = draw_prompt_ids(jax.random.fold_in(keys[6], 71), 0)
    return dict(hidden=hidden, lm_head=lm_head, reward_head=reward_head, target_ids=target_ids, lengths=lengths, prompt_ids=prompt_ids)


def reference(hidden, lm_head, reward_head, target_ids, lengths, prompt_ids):
    rows = hidden.reshape(TOKENS, D)
    wanted = target_ids.reshape(TOKENS)
    block = VOC_DEV * 8
    count = VOCAB // block

    def sweep(carry, index):
        peak, total, picked = carry
        start = (index * block).astype(jnp.int32)
        weights = lax.dynamic_slice_in_dim(lm_head, start, block, 1)
        logits = jnp.dot(rows, weights, preferred_element_type=jnp.float32)
        fresh = jnp.maximum(peak, lax.optimization_barrier(jnp.max(logits, axis=1)))
        total = total * jnp.exp(peak - fresh) + lax.optimization_barrier(jnp.sum(jnp.exp(logits - fresh[:, None]), axis=1))
        columns = start + lax.broadcasted_iota(jnp.int32, (1, block), 1)
        picked = picked + lax.optimization_barrier(jnp.sum(jnp.where(columns == wanted[:, None], logits, 0.0), axis=1))
        return ((fresh, total, picked), None)
    zeros = jnp.zeros((TOKENS,), jnp.float32)
    start_carry = (jnp.full((TOKENS,), -jnp.inf, jnp.float32), zeros, zeros)
    (peak, total, picked), _ = lax.scan(sweep, start_carry, jnp.arange(count, dtype=jnp.int32))
    logprob = (picked - (peak + jnp.log(total))).reshape(RESPONSES, WIN)
    positions = lax.broadcasted_iota(jnp.int32, (RESPONSES, WIN), 1)
    token_logprobs = jnp.where(positions < lengths[:, None], logprob, 0.0)
    last = jnp.take_along_axis(hidden, (lengths - 1).astype(jnp.int32)[:, None, None], axis=1)[:, 0, :]
    rewards = jnp.dot(last, reward_head, preferred_element_type=jnp.float32)
    member = (prompt_ids[:, None] == lax.broadcasted_iota(jnp.int32, (1, PROMPTS), 1)).astype(jnp.float32)
    sums = jnp.dot(rewards, member, precision=lax.Precision.HIGHEST)
    squares = jnp.dot(rewards * rewards, member, precision=lax.Precision.HIGHEST)
    means = sums / GROUP
    scales = jnp.sqrt(jnp.maximum(squares / GROUP - means * means, 1.0))
    centre = jnp.dot(member, means, precision=lax.Precision.HIGHEST)
    spread = jnp.dot(member, scales, precision=lax.Precision.HIGHEST)
    advantages = (rewards - centre) / spread
    return (token_logprobs, advantages)
```

```python
import functools

import jax
import jax.numpy as jnp
import numpy as np
from jax import lax
from jax.experimental import pallas as pl
from jax.experimental.pallas import tpu as pltpu
from jax.sharding import PartitionSpec as P

GROUP = 16
LANES = 128
ROWS = 256
AXES = ("rep", "dp")
VMEM = pltpu.VMEM


def bits_of(count):
    return [1 << k for k in range(count.bit_length() - 1)]


class Piece:
    def __init__(self, rows, tiles):
        self.rows = rows
        self.tiles = tiles


def swap(piece, masks, devices):
    pairs = [(i, i ^ masks[i & 1]) for i in range(devices)]
    rows = lax.ppermute(piece.rows, AXES, pairs)
    if masks == (1, 1):
        tiles = [(1 ^ b, 1 ^ a) for a, b in piece.tiles]
    else:
        tiles = [(a ^ masks[0], b ^ masks[1]) for a, b in piece.tiles]
    return Piece(rows, tiles)


def join(*pieces):
    return Piece(jnp.concatenate([p.rows for p in pieces], 0), sum((p.tiles for p in pieces), []))


def gather(own, rep, dp):
    devices = rep * dp
    inner = bits_of(dp)[1:]
    far, near = inner[-2:], inner[:-2]
    outer = [b * dp for b in bits_of(rep)]
    stages = []
    for k in range(max(len(near), len(outer))):
        pair = near[k : k + 1] + outer[k : k + 1]
        stages += [(pair[0], pair[-1]), (pair[-1], pair[0])][: len(pair)]
    hop = lambda piece, mask: swap(piece, (mask, mask), devices)
    z1, z2, z3 = hop(own, far[0]), hop(own, far[1]), hop(own, far[0] ^ far[1])
    done = []
    for group in (join(own, z1), join(z2, z3)):
        for masks in stages[:-1]:
            group = join(group, swap(group, masks, devices))
        last = swap(group, stages[-1], devices)
        done += [group, last]
    return done + [swap(p, (1, 1), devices) for p in done]


def split_ids(ids):
    tokens = ids.reshape(-1, 1)
    digits = [tokens & 255, (tokens >> 8) & 255, tokens >> 16]
    return jnp.concatenate(digits, 1).astype(jnp.bfloat16)


def iota(shape, axis):
    return lax.broadcasted_iota(jnp.int32, shape, axis)


def moments_kernel(hidden_ref, head_ref, lengths_ref, prompts_ref, sums_ref, member_ref, rewards_ref, *, start, prompts):
    resp, window, _ = hidden_ref.shape
    wide = sums_ref.shape[1]
    diag = iota((resp, resp), 0) == iota((resp, resp), 1)
    column = lambda ref: jnp.sum(jnp.where(diag, ref[...], 0), axis=1, keepdims=True)
    lengths, names = column(lengths_ref), column(prompts_ref)
    rows = hidden_ref[...].astype(jnp.float32)
    last = rows[:, 0, :]
    for w in range(1, window):
        last = jnp.where(lengths == w + 1, rows[:, w, :], last)
    rewards = jnp.sum(last * head_ref[...].astype(jnp.float32), axis=1, keepdims=True)
    lane = iota((resp, wide), 1)
    member_ref[...] = jnp.where(lane == names, 1.0, 0.0)
    first = jnp.where(lane == names + start, rewards, 0.0)
    second = jnp.where(lane == names + (start + prompts), rewards * rewards, 0.0)
    sums_ref[...] = jnp.sum(first + second, axis=0, keepdims=True)
    rewards_ref[...] = jnp.broadcast_to(rewards, rewards_ref.shape)


def stats_kernel(place_ref, me_ref, head_ref, sums_ref, *refs, window):
    pieces, message_ref, tiles_ref = refs[:-2], refs[-2], refs[-1]
    width, vocab = head_ref.shape
    devices, wide = message_ref.shape
    tokens = sum(p.shape[0] for p in pieces) // devices
    resp = tokens // window
    head = head_ref[...]
    base = (me_ref[0] * vocab).astype(jnp.float32)
    share = max(1, 8 // tokens)
    tile = tokens * share

    def block(piece, start, rows, first):
        part = piece[pl.ds(start, rows), :]
        logits = jnp.dot(part[:, :width], head, preferred_element_type=jnp.float32)
        digits = part[:, width : width + LANES].astype(jnp.float32)
        wanted = digits[:, 0:1] + 256.0 * digits[:, 1:2] + 65536.0 * digits[:, 2:3] - base
        columns = iota((rows, vocab), 1).astype(jnp.float32)
        peak = jnp.max(logits, axis=1, keepdims=True)
        total = jnp.sum(jnp.exp(logits - peak), axis=1, keepdims=True)
        picked = jnp.sum(jnp.where(columns == wanted, logits, 0.0), axis=1, keepdims=True)
        lane, token = iota((rows, wide), 1), iota((rows, wide), 0) % tokens
        slot = (token % window) * resp + token // window
        values = jnp.where(lane == slot, peak, 0.0)
        values = jnp.where(lane == slot + tokens, total, values)
        values = jnp.where(lane == slot + 2 * tokens, picked, values)
        values = values.reshape(rows // tile, tile, wide)
        for k in range(share):
            mine = values
            if share > 1:
                mine = jnp.where(iota(values.shape, 1) // tokens == k, values, 0.0)
            tiles_ref[k, pl.ds(first, rows // tile), :] = jnp.sum(mine, axis=1)

    first = 0
    for piece in pieces:
        count = piece.shape[0]
        rows = min(count, ROWS)
        if count == rows:
            block(piece, 0, rows, first)
        else:

            @pl.loop(0, count // rows)
            def _(i, piece=piece, rows=rows, first=first):
                block(
                    piece,
                    pl.multiple_of(i * rows, rows),
                    rows,
                    pl.multiple_of(first + i * (rows // tile), 8),
                )

        first += count // tile

    sums = sums_ref[...]

    def place(i):
        for k in range(share):
            message_ref[pl.ds(place_ref[i * share + k], 1), :] = tiles_ref[k, pl.ds(i, 1), :] + sums

    if devices <= 32:
        for i in range(devices // share):
            place(i)
    else:
        pl.loop(0, devices // share)(place)


def finish_kernel(message_ref, member_ref, rewards_ref, lengths_ref, logprobs_ref, advantages_ref, *, tokens, prompts):
    window, resp = logprobs_ref.shape
    message = message_ref[...]
    wide = message.shape[1]
    back = lambda x, by: pltpu.roll(x, (wide - by) % wide, 1)
    top = jnp.max(message, axis=0, keepdims=True)
    scaled = back(message, tokens) * jnp.exp(jnp.minimum(message - top, 0.0))
    total = jnp.sum(scaled, axis=0, keepdims=True)
    whole = jnp.sum(message, axis=0, keepdims=True)
    lane = iota((1, wide), 1)
    total = jnp.where(lane < tokens, total, 1.0)
    logprob = back(whole, 2 * tokens) - (top + jnp.log(total))
    for w in range(window):
        row = back(logprob, w * resp)[:, :resp] if w else logprob[:, :resp]
        logprobs_ref[w : w + 1, :] = jnp.where(w < lengths_ref[...], row, 0.0)
    means = back(whole, 3 * tokens) * (1.0 / GROUP)
    squares = back(whole, 3 * tokens + prompts) * (1.0 / GROUP)
    scales = jnp.sqrt(jnp.maximum(squares - means * means, 1.0))
    member = member_ref[...] > 0.5
    centre = jnp.sum(jnp.where(member, means, 0.0), axis=1, keepdims=True)
    spread = jnp.sum(jnp.where(member, scales, 0.0), axis=1, keepdims=True)
    advantages = (rewards_ref[:, 0:1] - centre) / spread
    diag = iota((resp, resp), 0) == iota((resp, resp), 1)
    advantages_ref[...] = jnp.sum(jnp.where(diag, advantages, 0.0), axis=0, keepdims=True)


def local(hidden, lm_head, reward_head, target_ids, lengths, prompt_ids):
    resp, window, width = hidden.shape
    vocab = lm_head.shape[1]
    rep, dp = lax.axis_size("rep"), lax.axis_size("dp")
    devices = rep * dp
    me = lax.axis_index("rep") * dp + lax.axis_index("dp")
    tokens = resp * window
    prompts = resp * devices // GROUP
    wide = -(-(3 * tokens + 2 * prompts) // LANES) * LANES
    f32 = jnp.float32

    extra = jnp.pad(split_ids(target_ids), ((0, 0), (0, LANES - 3)))
    own = jnp.concatenate([hidden.reshape(tokens, width), extra], 1)
    pieces = gather(Piece(own, [(0, 0)]), rep, dp)

    lengths_row, prompts_row = lengths.reshape(1, resp), prompt_ids.reshape(1, resp)
    sums, member, rewards = pl.pallas_call(
        functools.partial(moments_kernel, start=3 * tokens, prompts=prompts),
        out_shape=(
            jax.ShapeDtypeStruct((1, wide), f32),
            jax.ShapeDtypeStruct((resp, wide), f32),
            jax.ShapeDtypeStruct((resp, LANES), f32),
        ),
        name="moments",
    )(hidden, reward_head.reshape(1, width), lengths_row, prompts_row)

    marks = np.array(sum((p.tiles for p in pieces), []), np.int32)
    core = me & 1
    place = me ^ jnp.where(core == 0, marks[:, 0], marks[:, 1])
    share = max(1, 8 // tokens)
    smem = pl.BlockSpec(memory_space=pltpu.SMEM)
    vmem = pl.BlockSpec(memory_space=VMEM)
    message = pl.pallas_call(
        functools.partial(stats_kernel, window=window),
        out_shape=jax.ShapeDtypeStruct((devices, wide), f32),
        in_specs=[smem, smem] + [vmem] * (2 + len(pieces)),
        out_specs=vmem,
        scratch_shapes=[VMEM((share, devices // share, wide), f32)],
        name="stats",
    )(place, me.reshape(1), lm_head, sums, *[p.rows for p in pieces])

    answer = lax.all_to_all(message, AXES, 0, 0, tiled=True)
    logprobs, advantages = pl.pallas_call(
        functools.partial(finish_kernel, tokens=tokens, prompts=prompts),
        out_shape=(
            jax.ShapeDtypeStruct((window, resp), f32),
            jax.ShapeDtypeStruct((1, resp), f32),
        ),
        name="finish",
    )(answer, member, rewards, lengths_row)
    return (logprobs.T, advantages.reshape(resp))


def solution(mesh):
    in_specs = (
        P(("rep", "dp"), None, None),
        P(None, ("rep", "dp")),
        P(),
        P(("rep", "dp"), None),
        P(("rep", "dp")),
        P(("rep", "dp")),
    )
    out_specs = (P(("rep", "dp"), None), P(("rep", "dp")))
    return jax.shard_map(local, mesh=mesh, in_specs=in_specs, out_specs=out_specs, check_vma=False)
```

```python
import functools

import jax
import jax.numpy as jnp
from jax import lax
from jax.experimental import pallas as pl
from jax.experimental.pallas import tpu as pltpu
from jax.sharding import PartitionSpec as P


GROUP = 16
LANES = 128
ROWS = 256
SMALL = 4 << 20
MARGIN = 3 << 20
AXES = ("rep", "dp")
VMEM = pltpu.VMEM


def bits_of(count):
    return [1 << k for k in range(count.bit_length() - 1)]


class Piece:
    def __init__(self, rows, tiles):
        self.rows = rows
        self.tiles = tiles


def swap(piece, masks, devices):
    pairs = [(i, i ^ masks[i & 1]) for i in range(devices)]
    rows = lax.ppermute(piece.rows, AXES, pairs)
    if masks == (1, 1):
        tiles = [(1 ^ b, 1 ^ a) for a, b in piece.tiles]
    else:
        tiles = [(a ^ masks[0], b ^ masks[1]) for a, b in piece.tiles]
    return Piece(rows, tiles)


def join_kernel(*refs):
    *parts, out_ref = refs
    first = 0
    for part in parts:
        count = part.shape[0]
        out_ref[first : first + count, :] = part[...]
        first += count


def join(*pieces):
    count, width = sum(p.rows.shape[0] for p in pieces), pieces[0].rows.shape[1]
    vmem = pl.BlockSpec(memory_space=VMEM)
    rows = pl.pallas_call(
        join_kernel,
        out_shape=jax.ShapeDtypeStruct((count, width), pieces[0].rows.dtype),
        in_specs=[vmem] * len(pieces),
        out_specs=vmem,
        compiler_params=pltpu.CompilerParams(vmem_limit_bytes=SMALL + 4 * count * width),
        cost_estimate=pl.CostEstimate(flops=count * width, bytes_accessed=4 * count * width, transcendentals=0),
        name="join",
    )(*[p.rows for p in pieces])
    return Piece(rows, sum((p.tiles for p in pieces), []))


def gather(own, rep, dp):
    devices = rep * dp
    inner = bits_of(dp)[1:]
    far, near = inner[-2:], inner[:-2]
    outer = [b * dp for b in bits_of(rep)]
    stages = []
    for k in range(max(len(near), len(outer))):
        pair = near[k : k + 1] + outer[k : k + 1]
        stages += [(pair[0], pair[-1]), (pair[-1], pair[0])][: len(pair)]
    *before, one, two = stages
    for masks in before:
        own = join(own, swap(own, masks, devices))
    z1, z2 = [swap(own, (m, m), devices) for m in far]
    z3 = swap(z2, (far[0], far[0]), devices)
    own_1 = swap(own, one, devices)
    own_3 = swap(own, two, devices)
    own_2 = swap(join(z1, own_1), two, devices)
    near = join(own, z1, own_1, own_3)
    near_1 = swap(z1, one, devices)
    far_1 = swap(z2, one, devices)
    last_1 = swap(z3, one, devices)
    second = join(z2, near_1)
    second_2 = swap(second, two, devices)
    third = join(far_1, z3)
    third_2 = swap(third, two, devices)
    last_2 = swap(last_1, two, devices)
    buckets = [[near, own_2, second], [third, second_2], [last_1, third_2, last_2]]
    return [b + [swap(p, (1, 1), devices) for p in b] for b in buckets]


def iota(shape, axis):
    return lax.broadcasted_iota(jnp.int32, shape, axis)


def prepare_kernel(hidden_ref, names_ref, own_ref):
    resp, window, width = hidden_ref.shape
    tokens = resp * window
    own_ref[:, :width] = hidden_ref[...].reshape(tokens, width)
    lane, row = iota((tokens, resp), 1), iota((tokens, resp), 0)
    ids = names_ref[...]
    mine = jnp.zeros((tokens, resp), jnp.int32)
    for w in range(window):
        mine = jnp.where((row % window == w) & (row // window == lane), ids[w : w + 1, :], mine)
    mine = jnp.sum(mine, axis=1, keepdims=True)
    place = iota((tokens, LANES), 1)
    digits = jnp.where(place == 0, mine & 255, jnp.where(place == 1, (mine >> 8) & 255, mine >> 16))
    digits = jnp.where(place < 3, digits.astype(jnp.float32), 0.0)
    own_ref[:, width:] = digits.astype(jnp.bfloat16)


def moments_kernel(me_ref, own_ref, head_ref, names_ref, weights_ref, sums_ref, member_ref, rewards_ref, *, start, prompts):
    tokens = own_ref.shape[0]
    resp = member_ref.shape[0]
    window = tokens // resp
    wide = sums_ref.shape[1]
    lengths, prompt = names_ref[window : window + 1, :], names_ref[window + 1 : window + 2, :]
    parts = head_ref.shape[0]
    each = jnp.zeros((tokens, LANES), jnp.float32)
    for k in range(parts):
        rows = own_ref[:, k * LANES : (k + 1) * LANES].astype(jnp.float32)
        each += rows * head_ref[k : k + 1, :].astype(jnp.float32)
    each = jnp.sum(each, axis=1, keepdims=True)
    last = iota((tokens, resp), 0) == iota((tokens, resp), 1) * window + lengths - 1
    across = jnp.sum(jnp.where(last, each, 0.0), axis=0, keepdims=True)
    diag = iota((resp, resp), 0) == iota((resp, resp), 1)
    rewards = jnp.sum(jnp.where(diag, across, 0.0), axis=1, keepdims=True)
    named = jnp.sum(jnp.where(diag, prompt, 0), axis=1, keepdims=True)
    lane = iota((resp, wide), 1)
    member_ref[...] = jnp.where(lane == named, 1.0, 0.0)
    first = jnp.where(lane == named + start, rewards, 0.0)
    second = jnp.where(lane == named + (start + prompts), rewards * rewards, 0.0)
    sums_ref[...] = jnp.sum(first + second, axis=0, keepdims=True)
    rewards_ref[...] = jnp.broadcast_to(rewards, rewards_ref.shape)


def stats_block(part, head, base, window, tokens, wide):
    width, vocab = head.shape
    rows = part.shape[0]
    resp = tokens // window
    logits = jnp.dot(part[:, :width], head, preferred_element_type=jnp.float32)
    digits = part[:, width : width + LANES].astype(jnp.float32)
    wanted = digits[:, 0:1] + 256.0 * digits[:, 1:2] + 65536.0 * digits[:, 2:3] - base
    columns = iota((rows, vocab), 1).astype(jnp.float32)
    peak = jnp.max(logits, axis=1, keepdims=True)
    total = jnp.sum(jnp.exp(logits - peak), axis=1, keepdims=True)
    picked = jnp.sum(jnp.where(columns == wanted, logits, 0.0), axis=1, keepdims=True)
    lane, token = iota((rows, wide), 1), iota((rows, wide), 0) % tokens
    slot = (token % window) * resp + token // window
    values = jnp.where(lane == slot, peak, 0.0)
    values = jnp.where(lane == slot + tokens, total, values)
    values = jnp.where(lane == slot + 2 * tokens, picked, values)
    share = max(1, 8 // tokens)
    tile = tokens * share
    values = values.reshape(rows // tile, tile, wide)
    tiles = []
    for k in range(share):
        mine = values
        if share > 1:
            mine = jnp.where(iota(values.shape, 1) // tokens == k, values, 0.0)
        tiles.append(jnp.sum(mine, axis=1))
    return tiles


def stats_kernel(me_ref, head_ref, *refs, window, tokens, marks, early):
    if marks is None:
        pieces, tiles_ref = refs[:-1], refs[-1]
        wide = tiles_ref.shape[2]
    else:
        sums_ref, others, pieces, message_ref, tiles_ref = refs[0], refs[1 : 1 + early], refs[1 + early : -2], refs[-2], refs[-1]
        wide = message_ref.shape[1]
    share = max(1, 8 // tokens)
    tile = tokens * share
    vocab = head_ref.shape[1]
    me = me_ref[0]
    base = (me * vocab).astype(jnp.float32)
    limit = max(8 * tile, ROWS)

    def work(parts, first):
        part = parts[0] if len(parts) == 1 else jnp.concatenate(parts, 0)
        for k, rows in enumerate(stats_block(part, head_ref[...], base, window, tokens, wide)):
            tiles_ref[k, pl.ds(first, rows.shape[0]), :] = rows

    first, small = 0, []
    for piece in pieces:
        count = piece.shape[0]
        if sum(p.shape[0] for p in small) + count > limit and small:
            work([p[...] for p in small], first)
            first += sum(p.shape[0] for p in small) // tile
            small = []
        if count <= limit:
            small.append(piece)
            continue
        for i in range(count // limit):
            work([piece[i * limit : (i + 1) * limit, :]], first)
            first += limit // tile
    if small:
        work([p[...] for p in small], first)
    if marks is None:
        return

    sums = sums_ref[...]
    even = me % 2 == 0
    index = 0
    for ref in (*others, tiles_ref):
        for i in range(ref.shape[1]):
            for k in range(share):
                low, high = marks[index]
                row = me ^ (jnp.where(even, low, high) if low != high else low)
                message_ref[pl.ds(row, 1), :] = ref[k, i : i + 1, :] + sums
                index += 1


def finish_kernel(message_ref, member_ref, rewards_ref, names_ref, logprobs_ref, advantages_ref, *, tokens, prompts):
    window, resp = logprobs_ref.shape
    message = message_ref[...]
    wide = message.shape[1]
    back = lambda x, by: pltpu.roll(x, (wide - by) % wide, 1)
    top = jnp.max(message, axis=0, keepdims=True)
    scaled = back(message, tokens) * jnp.exp(jnp.minimum(message - top, 0.0))
    total = jnp.sum(scaled, axis=0, keepdims=True)
    whole = jnp.sum(message, axis=0, keepdims=True)
    lane = iota((1, wide), 1)
    total = jnp.where(lane < tokens, total, 1.0)
    logprob = back(whole, 2 * tokens) - (top + jnp.log(total))
    for w in range(window):
        row = back(logprob, w * resp)[:, :resp] if w else logprob[:, :resp]
        logprobs_ref[w : w + 1, :] = jnp.where(w < names_ref[window : window + 1, :], row, 0.0)
    means = back(whole, 3 * tokens) * (1.0 / GROUP)
    squares = back(whole, 3 * tokens + prompts) * (1.0 / GROUP)
    scales = jnp.sqrt(jnp.maximum(squares - means * means, 1.0))
    member = member_ref[...] > 0.5
    centre = jnp.sum(jnp.where(member, means, 0.0), axis=1, keepdims=True)
    spread = jnp.sum(jnp.where(member, scales, 0.0), axis=1, keepdims=True)
    advantages = (rewards_ref[:, 0:1] - centre) / spread
    diag = iota((resp, resp), 0) == iota((resp, resp), 1)
    advantages_ref[...] = jnp.sum(jnp.where(diag, advantages, 0.0), axis=0, keepdims=True)


def body(hidden, lm_head, reward_head, target_ids, lengths, prompt_ids):
    resp, window, width = hidden.shape
    vocab = lm_head.shape[1]
    rep, dp = lax.axis_size("rep"), lax.axis_size("dp")
    devices = rep * dp
    me = lax.axis_index("rep") * dp + lax.axis_index("dp")
    me = me.astype(jnp.int32).reshape(1)
    tokens = resp * window
    prompts = resp * devices // GROUP
    wide = -(-(3 * tokens + 2 * prompts) // LANES) * LANES
    share = max(1, 8 // tokens)
    f32 = jnp.float32
    smem = pl.BlockSpec(memory_space=pltpu.SMEM)
    vmem = pl.BlockSpec(memory_space=VMEM)

    names = jnp.concatenate([target_ids.T, lengths.reshape(1, resp), prompt_ids.reshape(1, resp)], 0)
    own = pl.pallas_call(
        prepare_kernel,
        out_shape=jax.ShapeDtypeStruct((tokens, width + LANES), jnp.bfloat16),
        compiler_params=pltpu.CompilerParams(vmem_limit_bytes=SMALL),
        name="prepare",
    )(hidden, names)
    buckets = gather(Piece(own, [(0, 0)]), rep, dp)

    sums, member, rewards = pl.pallas_call(
        functools.partial(moments_kernel, start=3 * tokens, prompts=prompts),
        out_shape=(
            jax.ShapeDtypeStruct((1, wide), f32),
            jax.ShapeDtypeStruct((resp, wide), f32),
            jax.ShapeDtypeStruct((resp, LANES), f32),
        ),
        in_specs=[smem] + [vmem] * 4,
        out_specs=[vmem] * 3,
        compiler_params=pltpu.CompilerParams(vmem_limit_bytes=SMALL),
        cost_estimate=pl.CostEstimate(flops=10**7, bytes_accessed=2 * hidden.size, transcendentals=0),
        name="moments",
    )(me, own, reward_head.reshape(width // LANES, LANES), names, lm_head)

    marks = [m for b in buckets for p in b for m in p.tiles]

    def stats(bucket, early):
        count = sum(p.rows.shape[0] for p in bucket)
        tiles = (share, count // tokens // share, wide)
        last = early is not None
        given = [sums, *early] if last else []
        cost = pl.CostEstimate(flops=2 * count * lm_head.size, bytes_accessed=2 * lm_head.size, transcendentals=count * vocab)
        return pl.pallas_call(
            functools.partial(stats_kernel, window=window, tokens=tokens, marks=marks if last else None, early=len(given) - 1),
            out_shape=jax.ShapeDtypeStruct((devices, wide) if last else tiles, f32),
            in_specs=[smem] + [vmem] * (1 + len(given) + len(bucket)),
            out_specs=vmem,
            scratch_shapes=[VMEM(tiles, f32)] if last else [],
            compiler_params=pltpu.CompilerParams(vmem_limit_bytes=MARGIN + 2 * lm_head.size + 2 * count * (width + LANES)),
            cost_estimate=cost,
            name="stats",
        )(me, lm_head, *given, *[p.rows for p in bucket])

    early = [stats(b, None) for b in buckets[:-1]]
    message = stats(buckets[-1], early)
    answer = lax.all_to_all(message, AXES, 0, 0, tiled=True)
    logprobs, advantages = pl.pallas_call(
        functools.partial(finish_kernel, tokens=tokens, prompts=prompts),
        out_shape=(
            jax.ShapeDtypeStruct((window, resp), f32),
            jax.ShapeDtypeStruct((1, resp), f32),
        ),
        compiler_params=pltpu.CompilerParams(vmem_limit_bytes=SMALL),
        name="finish",
    )(answer, member, rewards, names)
    return (logprobs.T, advantages.reshape(resp))


def solution(mesh):
    in_specs = (
        P(("rep", "dp"), None, None),
        P(None, ("rep", "dp")),
        P(),
        P(("rep", "dp"), None),
        P(("rep", "dp")),
        P(("rep", "dp")),
    )
    out_specs = (P(("rep", "dp"), None), P(("rep", "dp")))
    return jax.shard_map(body, mesh=mesh, in_specs=in_specs, out_specs=out_specs, check_vma=False)
```

```python
import functools

import jax
import jax.numpy as jnp
from jax import lax
from jax.experimental import pallas as pl
from jax.experimental.pallas import tpu as pltpu
from jax.sharding import PartitionSpec as P


GROUP = 16
LANES = 128
ROWS = 256
SMALL = 4 << 20
MARGIN = 3 << 20
AXES = ("rep", "dp")
VMEM = pltpu.VMEM


def bits_of(count):
    return [1 << k for k in range(count.bit_length() - 1)]


class Piece:
    def __init__(self, rows, tiles):
        self.rows = rows
        self.tiles = tiles


def swap(piece, masks, devices):
    pairs = [(i, i ^ masks[i & 1]) for i in range(devices)]
    rows = lax.ppermute(piece.rows, AXES, pairs)
    if masks == (1, 1):
        tiles = [(1 ^ b, 1 ^ a) for a, b in piece.tiles]
    else:
        tiles = [(a ^ masks[0], b ^ masks[1]) for a, b in piece.tiles]
    return Piece(rows, tiles)


def join_kernel(*refs):
    *parts, out_ref = refs
    first = 0
    for part in parts:
        count = part.shape[0]
        out_ref[first : first + count, :] = part[...]
        first += count


def join(*pieces):
    count, width = sum(p.rows.shape[0] for p in pieces), pieces[0].rows.shape[1]
    vmem = pl.BlockSpec(memory_space=VMEM)
    rows = pl.pallas_call(
        join_kernel,
        out_shape=jax.ShapeDtypeStruct((count, width), pieces[0].rows.dtype),
        in_specs=[vmem] * len(pieces),
        out_specs=vmem,
        compiler_params=pltpu.CompilerParams(vmem_limit_bytes=SMALL + 4 * count * width),
        cost_estimate=pl.CostEstimate(flops=count * width, bytes_accessed=4 * count * width, transcendentals=0),
        name="join",
    )(*[p.rows for p in pieces])
    return Piece(rows, sum((p.tiles for p in pieces), []))


def gather(own, rep, dp):
    devices = rep * dp
    inner = bits_of(dp)[1:]
    far, near = inner[-2:], inner[:-2]
    outer = [b * dp for b in bits_of(rep)]
    stages = []
    for k in range(max(len(near), len(outer))):
        pair = near[k : k + 1] + outer[k : k + 1]
        stages += [(pair[0], pair[-1]), (pair[-1], pair[0])][: len(pair)]
    *before, one, two = stages
    for masks in before:
        own = join(own, swap(own, masks, devices))
    z1, z2 = [swap(own, (m, m), devices) for m in far]
    z3 = swap(z2, (far[0], far[0]), devices)
    own_1 = swap(own, one, devices)
    own_3 = swap(own, two, devices)
    own_2 = swap(join(z1, own_1), two, devices)
    near = join(own, z1, own_1, own_3)
    near_1 = swap(z1, one, devices)
    far_1 = swap(z2, one, devices)
    last_1 = swap(z3, one, devices)
    far_3 = swap(z2, two, devices)
    third = join(near_1, far_1, z3)
    third_2 = swap(third, two, devices)
    last_2 = swap(last_1, two, devices)
    with_z2 = join(z2, far_3, third, last_1)
    buckets = [[near, own_2], [with_z2], [third_2, last_2]]
    return [b + [swap(p, (1, 1), devices) for p in b] for b in buckets]


def iota(shape, axis):
    return lax.broadcasted_iota(jnp.int32, shape, axis)


def prepare_kernel(hidden_ref, names_ref, own_ref):
    resp, window, width = hidden_ref.shape
    tokens = resp * window
    own_ref[:, :width] = hidden_ref[...].reshape(tokens, width)
    lane, row = iota((tokens, resp), 1), iota((tokens, resp), 0)
    ids = names_ref[...]
    mine = jnp.zeros((tokens, resp), jnp.int32)
    for w in range(window):
        mine = jnp.where((row % window == w) & (row // window == lane), ids[w : w + 1, :], mine)
    mine = jnp.sum(mine, axis=1, keepdims=True)
    place = iota((tokens, LANES), 1)
    digits = jnp.where(place == 0, mine & 255, jnp.where(place == 1, (mine >> 8) & 255, mine >> 16))
    digits = jnp.where(place < 3, digits.astype(jnp.float32), 0.0)
    own_ref[:, width:] = digits.astype(jnp.bfloat16)


def moments_kernel(me_ref, own_ref, head_ref, names_ref, weights_ref, sums_ref, member_ref, rewards_ref, *, start, prompts):
    tokens = own_ref.shape[0]
    resp = member_ref.shape[0]
    window = tokens // resp
    wide = sums_ref.shape[1]
    lengths, prompt = names_ref[window : window + 1, :], names_ref[window + 1 : window + 2, :]
    parts = head_ref.shape[0]
    each = jnp.zeros((tokens, LANES), jnp.float32)
    for k in range(parts):
        rows = own_ref[:, k * LANES : (k + 1) * LANES].astype(jnp.float32)
        each += rows * head_ref[k : k + 1, :].astype(jnp.float32)
    each = jnp.sum(each, axis=1, keepdims=True)
    last = iota((tokens, resp), 0) == iota((tokens, resp), 1) * window + lengths - 1
    across = jnp.sum(jnp.where(last, each, 0.0), axis=0, keepdims=True)
    diag = iota((resp, resp), 0) == iota((resp, resp), 1)
    rewards = jnp.sum(jnp.where(diag, across, 0.0), axis=1, keepdims=True)
    named = jnp.sum(jnp.where(diag, prompt, 0), axis=1, keepdims=True)
    lane = iota((resp, wide), 1)
    member_ref[...] = jnp.where(lane == named, 1.0, 0.0)
    first = jnp.where(lane == named + start, rewards, 0.0)
    second = jnp.where(lane == named + (start + prompts), rewards * rewards, 0.0)
    sums_ref[...] = jnp.sum(first + second, axis=0, keepdims=True)
    rewards_ref[...] = jnp.broadcast_to(rewards, rewards_ref.shape)


def stats_block(part, head, base, window, tokens, wide):
    width, vocab = head.shape
    rows = part.shape[0]
    resp = tokens // window
    logits = jnp.dot(part[:, :width], head, preferred_element_type=jnp.float32)
    digits = part[:, width : width + LANES].astype(jnp.float32)
    wanted = digits[:, 0:1] + 256.0 * digits[:, 1:2] + 65536.0 * digits[:, 2:3] - base
    columns = iota((rows, vocab), 1).astype(jnp.float32)
    peak = jnp.max(logits, axis=1, keepdims=True)
    total = jnp.sum(jnp.exp(logits - peak), axis=1, keepdims=True)
    picked = jnp.sum(jnp.where(columns == wanted, logits, 0.0), axis=1, keepdims=True)
    lane, token = iota((rows, wide), 1), iota((rows, wide), 0) % tokens
    slot = (token % window) * resp + token // window
    values = jnp.where(lane == slot, peak, 0.0)
    values = jnp.where(lane == slot + tokens, total, values)
    values = jnp.where(lane == slot + 2 * tokens, picked, values)
    share = max(1, 8 // tokens)
    tile = tokens * share
    values = values.reshape(rows // tile, tile, wide)
    tiles = []
    for k in range(share):
        mine = values
        if share > 1:
            mine = jnp.where(iota(values.shape, 1) // tokens == k, values, 0.0)
        tiles.append(jnp.sum(mine, axis=1))
    return tiles


def stats_kernel(me_ref, head_ref, *refs, window, tokens, marks, early):
    if marks is None:
        pieces, tiles_ref = refs[:-1], refs[-1]
        wide = tiles_ref.shape[2]
    else:
        sums_ref, others, pieces, message_ref, tiles_ref = refs[0], refs[1 : 1 + early], refs[1 + early : -2], refs[-2], refs[-1]
        wide = message_ref.shape[1]
    share = max(1, 8 // tokens)
    tile = tokens * share
    vocab = head_ref.shape[1]
    me = me_ref[0]
    base = (me * vocab).astype(jnp.float32)
    limit = max(8 * tile, ROWS)

    def work(parts, first):
        part = parts[0] if len(parts) == 1 else jnp.concatenate(parts, 0)
        for k, rows in enumerate(stats_block(part, head_ref[...], base, window, tokens, wide)):
            tiles_ref[k, pl.ds(first, rows.shape[0]), :] = rows

    first, small = 0, []
    for piece in pieces:
        count = piece.shape[0]
        if sum(p.shape[0] for p in small) + count > limit and small:
            work([p[...] for p in small], first)
            first += sum(p.shape[0] for p in small) // tile
            small = []
        if count <= limit:
            small.append(piece)
            continue
        for i in range(count // limit):
            work([piece[i * limit : (i + 1) * limit, :]], first)
            first += limit // tile
    if small:
        work([p[...] for p in small], first)
    if marks is None:
        return

    sums = sums_ref[...]
    even = me % 2 == 0
    index = 0
    for ref in (*others, tiles_ref):
        for i in range(ref.shape[1]):
            for k in range(share):
                low, high = marks[index]
                row = me ^ (jnp.where(even, low, high) if low != high else low)
                message_ref[pl.ds(row, 1), :] = ref[k, i : i + 1, :] + sums
                index += 1


def finish_kernel(message_ref, member_ref, rewards_ref, names_ref, logprobs_ref, advantages_ref, *, tokens, prompts):
    window, resp = logprobs_ref.shape
    message = message_ref[...]
    wide = message.shape[1]
    back = lambda x, by: pltpu.roll(x, (wide - by) % wide, 1)
    top = jnp.max(message, axis=0, keepdims=True)
    scaled = back(message, tokens) * jnp.exp(jnp.minimum(message - top, 0.0))
    total = jnp.sum(scaled, axis=0, keepdims=True)
    whole = jnp.sum(message, axis=0, keepdims=True)
    lane = iota((1, wide), 1)
    total = jnp.where(lane < tokens, total, 1.0)
    logprob = back(whole, 2 * tokens) - (top + jnp.log(total))
    for w in range(window):
        row = back(logprob, w * resp)[:, :resp] if w else logprob[:, :resp]
        logprobs_ref[w : w + 1, :] = jnp.where(w < names_ref[window : window + 1, :], row, 0.0)
    means = back(whole, 3 * tokens) * (1.0 / GROUP)
    squares = back(whole, 3 * tokens + prompts) * (1.0 / GROUP)
    scales = jnp.sqrt(jnp.maximum(squares - means * means, 1.0))
    member = member_ref[...] > 0.5
    centre = jnp.sum(jnp.where(member, means, 0.0), axis=1, keepdims=True)
    spread = jnp.sum(jnp.where(member, scales, 0.0), axis=1, keepdims=True)
    advantages = (rewards_ref[:, 0:1] - centre) / spread
    diag = iota((resp, resp), 0) == iota((resp, resp), 1)
    advantages_ref[...] = jnp.sum(jnp.where(diag, advantages, 0.0), axis=0, keepdims=True)


def body(hidden, lm_head, reward_head, target_ids, lengths, prompt_ids):
    resp, window, width = hidden.shape
    vocab = lm_head.shape[1]
    rep, dp = lax.axis_size("rep"), lax.axis_size("dp")
    devices = rep * dp
    me = lax.axis_index("rep") * dp + lax.axis_index("dp")
    me = me.astype(jnp.int32).reshape(1)
    tokens = resp * window
    prompts = resp * devices // GROUP
    wide = -(-(3 * tokens + 2 * prompts) // LANES) * LANES
    share = max(1, 8 // tokens)
    f32 = jnp.float32
    smem = pl.BlockSpec(memory_space=pltpu.SMEM)
    vmem = pl.BlockSpec(memory_space=VMEM)

    names = jnp.concatenate([target_ids.T, lengths.reshape(1, resp), prompt_ids.reshape(1, resp)], 0)
    own = pl.pallas_call(
        prepare_kernel,
        out_shape=jax.ShapeDtypeStruct((tokens, width + LANES), jnp.bfloat16),
        compiler_params=pltpu.CompilerParams(vmem_limit_bytes=SMALL),
        name="prepare",
    )(hidden, names)
    buckets = gather(Piece(own, [(0, 0)]), rep, dp)

    sums, member, rewards = pl.pallas_call(
        functools.partial(moments_kernel, start=3 * tokens, prompts=prompts),
        out_shape=(
            jax.ShapeDtypeStruct((1, wide), f32),
            jax.ShapeDtypeStruct((resp, wide), f32),
            jax.ShapeDtypeStruct((resp, LANES), f32),
        ),
        in_specs=[smem] + [vmem] * 4,
        out_specs=[vmem] * 3,
        compiler_params=pltpu.CompilerParams(vmem_limit_bytes=SMALL),
        cost_estimate=pl.CostEstimate(flops=10**7, bytes_accessed=2 * hidden.size, transcendentals=0),
        name="moments",
    )(me, own, reward_head.reshape(width // LANES, LANES), names, lm_head)

    marks = [m for b in buckets for p in b for m in p.tiles]

    def stats(bucket, early):
        count = sum(p.rows.shape[0] for p in bucket)
        tiles = (share, count // tokens // share, wide)
        last = early is not None
        given = [sums, *early] if last else []
        cost = pl.CostEstimate(flops=2 * count * lm_head.size, bytes_accessed=2 * lm_head.size, transcendentals=count * vocab)
        return pl.pallas_call(
            functools.partial(stats_kernel, window=window, tokens=tokens, marks=marks if last else None, early=len(given) - 1),
            out_shape=jax.ShapeDtypeStruct((devices, wide) if last else tiles, f32),
            in_specs=[smem] + [vmem] * (1 + len(given) + len(bucket)),
            out_specs=vmem,
            scratch_shapes=[VMEM(tiles, f32)] if last else [],
            compiler_params=pltpu.CompilerParams(vmem_limit_bytes=MARGIN + 2 * lm_head.size + 2 * count * (width + LANES)),
            cost_estimate=cost,
            name="stats",
        )(me, lm_head, *given, *[p.rows for p in bucket])

    early = [stats(b, None) for b in buckets[:-1]]
    message = stats(buckets[-1], early)
    answer = lax.all_to_all(message, AXES, 0, 0, tiled=True)
    logprobs, advantages = pl.pallas_call(
        functools.partial(finish_kernel, tokens=tokens, prompts=prompts),
        out_shape=(
            jax.ShapeDtypeStruct((window, resp), f32),
            jax.ShapeDtypeStruct((1, resp), f32),
        ),
        compiler_params=pltpu.CompilerParams(vmem_limit_bytes=SMALL),
        name="finish",
    )(answer, member, rewards, names)
    return (logprobs.T, advantages.reshape(resp))


def solution(mesh):
    in_specs = (
        P(("rep", "dp"), None, None),
        P(None, ("rep", "dp")),
        P(),
        P(("rep", "dp"), None),
        P(("rep", "dp")),
        P(("rep", "dp")),
    )
    out_specs = (P(("rep", "dp"), None), P(("rep", "dp")))
    return jax.shard_map(body, mesh=mesh, in_specs=in_specs, out_specs=out_specs, check_vma=False)
```

```python
import functools

import jax
import jax.numpy as jnp
from jax import lax
from jax.experimental import pallas as pl
from jax.experimental.pallas import tpu as pltpu
from jax.sharding import PartitionSpec as P


GROUP = 16
LANES = 128
ROWS = 256
SMALL = 4 << 20
MARGIN = 3 << 20
AXES = ("rep", "dp")
VMEM = pltpu.VMEM


def bits_of(count):
    return [1 << k for k in range(count.bit_length() - 1)]


class Piece:
    def __init__(self, rows, tiles):
        self.rows = rows
        self.tiles = tiles


def swap(piece, masks, devices):
    pairs = [(i, i ^ masks[i & 1]) for i in range(devices)]
    rows = lax.ppermute(piece.rows, AXES, pairs)
    if masks == (1, 1):
        tiles = [(1 ^ b, 1 ^ a) for a, b in piece.tiles]
    else:
        tiles = [(a ^ masks[0], b ^ masks[1]) for a, b in piece.tiles]
    return Piece(rows, tiles)


def join_kernel(*refs):
    *parts, out_ref = refs
    first = 0
    for part in parts:
        count = part.shape[0]
        out_ref[first : first + count, :] = part[...]
        first += count


def join(*pieces):
    count, width = sum(p.rows.shape[0] for p in pieces), pieces[0].rows.shape[1]
    vmem = pl.BlockSpec(memory_space=VMEM)
    rows = pl.pallas_call(
        join_kernel,
        out_shape=jax.ShapeDtypeStruct((count, width), pieces[0].rows.dtype),
        in_specs=[vmem] * len(pieces),
        out_specs=vmem,
        compiler_params=pltpu.CompilerParams(vmem_limit_bytes=SMALL + 4 * count * width),
        cost_estimate=pl.CostEstimate(flops=count * width, bytes_accessed=4 * count * width, transcendentals=0),
        name="join",
    )(*[p.rows for p in pieces])
    return Piece(rows, sum((p.tiles for p in pieces), []))


def gather(own, rep, dp):
    devices = rep * dp
    inner = bits_of(dp)[1:]
    far, near = inner[-2:], inner[:-2]
    outer = [b * dp for b in bits_of(rep)]
    stages = []
    for k in range(max(len(near), len(outer))):
        pair = near[k : k + 1] + outer[k : k + 1]
        stages += [(pair[-1], pair[0]), (pair[0], pair[-1])][: len(pair)]
    *before, one, two = stages
    for masks in before:
        own = join(own, swap(own, masks, devices))
    z1, z2 = [swap(own, (m, m), devices) for m in far]
    z3 = swap(z2, (far[0], far[0]), devices)
    own_1 = swap(own, one, devices)
    own_3 = swap(own, two, devices)
    own_2 = swap(join(z1, own_1), two, devices)
    near = join(own, z1, own_1, own_3)
    near_1 = swap(z1, one, devices)
    far_1 = swap(z2, one, devices)
    last_1 = swap(z3, one, devices)
    far_3 = swap(z2, two, devices)
    near_2 = swap(near_1, two, devices)
    third = join(far_1, z3)
    third_2 = swap(third, two, devices)
    last_2 = swap(last_1, two, devices)
    with_z2 = join(z2, far_3, near_1, near_2, third, last_1)
    buckets = [[near, own_2], [with_z2], [third_2, last_2]]
    return [b + [swap(p, (1, 1), devices) for p in b] for b in buckets]


def iota(shape, axis):
    return lax.broadcasted_iota(jnp.int32, shape, axis)


def prepare_kernel(hidden_ref, names_ref, own_ref):
    resp, window, width = hidden_ref.shape
    tokens = resp * window
    own_ref[:, :width] = hidden_ref[...].reshape(tokens, width)
    lane, row = iota((tokens, resp), 1), iota((tokens, resp), 0)
    ids = names_ref[...]
    mine = jnp.zeros((tokens, resp), jnp.int32)
    for w in range(window):
        mine = jnp.where((row % window == w) & (row // window == lane), ids[w : w + 1, :], mine)
    mine = jnp.sum(mine, axis=1, keepdims=True)
    place = iota((tokens, LANES), 1)
    digits = jnp.where(place == 0, mine & 255, jnp.where(place == 1, (mine >> 8) & 255, mine >> 16))
    digits = jnp.where(place < 3, digits.astype(jnp.float32), 0.0)
    own_ref[:, width:] = digits.astype(jnp.bfloat16)


def moments_kernel(me_ref, own_ref, head_ref, names_ref, weights_ref, sums_ref, member_ref, rewards_ref, *, start, prompts):
    tokens = own_ref.shape[0]
    resp = member_ref.shape[0]
    window = tokens // resp
    wide = sums_ref.shape[1]
    lengths, prompt = names_ref[window : window + 1, :], names_ref[window + 1 : window + 2, :]
    parts = head_ref.shape[0]
    each = jnp.zeros((tokens, LANES), jnp.float32)
    for k in range(parts):
        rows = own_ref[:, k * LANES : (k + 1) * LANES].astype(jnp.float32)
        each += rows * head_ref[k : k + 1, :].astype(jnp.float32)
    each = jnp.sum(each, axis=1, keepdims=True)
    last = iota((tokens, resp), 0) == iota((tokens, resp), 1) * window + lengths - 1
    across = jnp.sum(jnp.where(last, each, 0.0), axis=0, keepdims=True)
    diag = iota((resp, resp), 0) == iota((resp, resp), 1)
    rewards = jnp.sum(jnp.where(diag, across, 0.0), axis=1, keepdims=True)
    named = jnp.sum(jnp.where(diag, prompt, 0), axis=1, keepdims=True)
    lane = iota((resp, wide), 1)
    member_ref[...] = jnp.where(lane == named, 1.0, 0.0)
    first = jnp.where(lane == named + start, rewards, 0.0)
    second = jnp.where(lane == named + (start + prompts), rewards * rewards, 0.0)
    sums_ref[...] = jnp.sum(first + second, axis=0, keepdims=True)
    rewards_ref[...] = jnp.broadcast_to(rewards, rewards_ref.shape)


def stats_block(part, head, base, window, tokens, wide):
    width, vocab = head.shape
    rows = part.shape[0]
    resp = tokens // window
    logits = jnp.dot(part[:, :width], head, preferred_element_type=jnp.float32)
    digits = part[:, width : width + LANES].astype(jnp.float32)
    wanted = digits[:, 0:1] + 256.0 * digits[:, 1:2] + 65536.0 * digits[:, 2:3] - base
    columns = iota((rows, vocab), 1).astype(jnp.float32)
    peak = jnp.max(logits, axis=1, keepdims=True)
    total = jnp.sum(jnp.exp(logits - peak), axis=1, keepdims=True)
    picked = jnp.sum(jnp.where(columns == wanted, logits, 0.0), axis=1, keepdims=True)
    lane, token = iota((rows, wide), 1), iota((rows, wide), 0) % tokens
    slot = (token % window) * resp + token // window
    values = jnp.where(lane == slot, peak, 0.0)
    values = jnp.where(lane == slot + tokens, total, values)
    values = jnp.where(lane == slot + 2 * tokens, picked, values)
    share = max(1, 8 // tokens)
    tile = tokens * share
    values = values.reshape(rows // tile, tile, wide)
    tiles = []
    for k in range(share):
        mine = values
        if share > 1:
            mine = jnp.where(iota(values.shape, 1) // tokens == k, values, 0.0)
        tiles.append(jnp.sum(mine, axis=1))
    return tiles


def stats_kernel(me_ref, head_ref, *refs, window, tokens, marks, early):
    if marks is None:
        pieces, tiles_ref = refs[:-1], refs[-1]
        wide = tiles_ref.shape[2]
    else:
        sums_ref, others, pieces, message_ref, tiles_ref = refs[0], refs[1 : 1 + early], refs[1 + early : -2], refs[-2], refs[-1]
        wide = message_ref.shape[1]
    share = max(1, 8 // tokens)
    tile = tokens * share
    vocab = head_ref.shape[1]
    me = me_ref[0]
    base = (me * vocab).astype(jnp.float32)
    limit = max(8 * tile, ROWS)

    def work(parts, first):
        part = parts[0] if len(parts) == 1 else jnp.concatenate(parts, 0)
        for k, rows in enumerate(stats_block(part, head_ref[...], base, window, tokens, wide)):
            tiles_ref[k, pl.ds(first, rows.shape[0]), :] = rows

    first, small = 0, []
    for piece in pieces:
        count = piece.shape[0]
        if sum(p.shape[0] for p in small) + count > limit and small:
            work([p[...] for p in small], first)
            first += sum(p.shape[0] for p in small) // tile
            small = []
        if count <= limit:
            small.append(piece)
            continue
        for i in range(count // limit):
            work([piece[i * limit : (i + 1) * limit, :]], first)
            first += limit // tile
    if small:
        work([p[...] for p in small], first)
    if marks is None:
        return

    sums = sums_ref[...]
    even = me % 2 == 0
    index = 0
    for ref in (*others, tiles_ref):
        for i in range(ref.shape[1]):
            for k in range(share):
                low, high = marks[index]
                row = me ^ (jnp.where(even, low, high) if low != high else low)
                message_ref[pl.ds(row, 1), :] = ref[k, i : i + 1, :] + sums
                index += 1


def finish_kernel(message_ref, member_ref, rewards_ref, names_ref, logprobs_ref, advantages_ref, *, tokens, prompts):
    window, resp = logprobs_ref.shape
    message = message_ref[...]
    wide = message.shape[1]
    back = lambda x, by: pltpu.roll(x, (wide - by) % wide, 1)
    top = jnp.max(message, axis=0, keepdims=True)
    scaled = back(message, tokens) * jnp.exp(jnp.minimum(message - top, 0.0))
    total = jnp.sum(scaled, axis=0, keepdims=True)
    whole = jnp.sum(message, axis=0, keepdims=True)
    lane = iota((1, wide), 1)
    total = jnp.where(lane < tokens, total, 1.0)
    logprob = back(whole, 2 * tokens) - (top + jnp.log(total))
    for w in range(window):
        row = back(logprob, w * resp)[:, :resp] if w else logprob[:, :resp]
        logprobs_ref[w : w + 1, :] = jnp.where(w < names_ref[window : window + 1, :], row, 0.0)
    means = back(whole, 3 * tokens) * (1.0 / GROUP)
    squares = back(whole, 3 * tokens + prompts) * (1.0 / GROUP)
    scales = jnp.sqrt(jnp.maximum(squares - means * means, 1.0))
    member = member_ref[...] > 0.5
    centre = jnp.sum(jnp.where(member, means, 0.0), axis=1, keepdims=True)
    spread = jnp.sum(jnp.where(member, scales, 0.0), axis=1, keepdims=True)
    advantages = (rewards_ref[:, 0:1] - centre) / spread
    diag = iota((resp, resp), 0) == iota((resp, resp), 1)
    advantages_ref[...] = jnp.sum(jnp.where(diag, advantages, 0.0), axis=0, keepdims=True)


def body(hidden, lm_head, reward_head, target_ids, lengths, prompt_ids):
    resp, window, width = hidden.shape
    vocab = lm_head.shape[1]
    rep, dp = lax.axis_size("rep"), lax.axis_size("dp")
    devices = rep * dp
    me = lax.axis_index("rep") * dp + lax.axis_index("dp")
    me = me.astype(jnp.int32).reshape(1)
    tokens = resp * window
    prompts = resp * devices // GROUP
    wide = -(-(3 * tokens + 2 * prompts) // LANES) * LANES
    share = max(1, 8 // tokens)
    f32 = jnp.float32
    smem = pl.BlockSpec(memory_space=pltpu.SMEM)
    vmem = pl.BlockSpec(memory_space=VMEM)

    names = jnp.concatenate([target_ids.T, lengths.reshape(1, resp), prompt_ids.reshape(1, resp)], 0)
    own = pl.pallas_call(
        prepare_kernel,
        out_shape=jax.ShapeDtypeStruct((tokens, width + LANES), jnp.bfloat16),
        compiler_params=pltpu.CompilerParams(vmem_limit_bytes=SMALL),
        name="prepare",
    )(hidden, names)
    buckets = gather(Piece(own, [(0, 0)]), rep, dp)

    sums, member, rewards = pl.pallas_call(
        functools.partial(moments_kernel, start=3 * tokens, prompts=prompts),
        out_shape=(
            jax.ShapeDtypeStruct((1, wide), f32),
            jax.ShapeDtypeStruct((resp, wide), f32),
            jax.ShapeDtypeStruct((resp, LANES), f32),
        ),
        in_specs=[smem] + [vmem] * 4,
        out_specs=[vmem] * 3,
        compiler_params=pltpu.CompilerParams(vmem_limit_bytes=SMALL),
        cost_estimate=pl.CostEstimate(flops=10**7, bytes_accessed=2 * hidden.size, transcendentals=0),
        name="moments",
    )(me, own, reward_head.reshape(width // LANES, LANES), names, lm_head)

    marks = [m for b in buckets for p in b for m in p.tiles]

    def stats(bucket, early):
        count = sum(p.rows.shape[0] for p in bucket)
        tiles = (share, count // tokens // share, wide)
        last = early is not None
        given = [sums, *early] if last else []
        cost = pl.CostEstimate(flops=2 * count * lm_head.size, bytes_accessed=2 * lm_head.size, transcendentals=count * vocab)
        return pl.pallas_call(
            functools.partial(stats_kernel, window=window, tokens=tokens, marks=marks if last else None, early=len(given) - 1),
            out_shape=jax.ShapeDtypeStruct((devices, wide) if last else tiles, f32),
            in_specs=[smem] + [vmem] * (1 + len(given) + len(bucket)),
            out_specs=vmem,
            scratch_shapes=[VMEM(tiles, f32)] if last else [],
            compiler_params=pltpu.CompilerParams(vmem_limit_bytes=MARGIN + 2 * lm_head.size + 2 * count * (width + LANES)),
            cost_estimate=cost,
            name="stats",
        )(me, lm_head, *given, *[p.rows for p in bucket])

    early = [stats(b, None) for b in buckets[:-1]]
    message = stats(buckets[-1], early)
    answer = lax.all_to_all(message, AXES, 0, 0, tiled=True)
    logprobs, advantages = pl.pallas_call(
        functools.partial(finish_kernel, tokens=tokens, prompts=prompts),
        out_shape=(
            jax.ShapeDtypeStruct((window, resp), f32),
            jax.ShapeDtypeStruct((1, resp), f32),
        ),
        compiler_params=pltpu.CompilerParams(vmem_limit_bytes=SMALL),
        name="finish",
    )(answer, member, rewards, names)
    return (logprobs.T, advantages.reshape(resp))


def solution(mesh):
    in_specs = (
        P(("rep", "dp"), None, None),
        P(None, ("rep", "dp")),
        P(),
        P(("rep", "dp"), None),
        P(("rep", "dp")),
        P(("rep", "dp")),
    )
    out_specs = (P(("rep", "dp"), None), P(("rep", "dp")))
    return jax.shard_map(body, mesh=mesh, in_specs=in_specs, out_specs=out_specs, check_vma=False)
```
